32 devices in a mesh: stage: 4 (over z), data: 8 (over y, x, core).
Axes of the slice: x: 2, y: 2, z: 4, core: 2. Of those that a mesh axis runs over, the one named last changes fastest.
Arguments:
- inputs: bfloat16 [32, 64, 896], P('data')
- targets: bfloat16 [32, 64, 896], P('data')
- w_up: bfloat16 [12, 896, 4864], P('stage')
- w_down: bfloat16 [12, 4864, 896], P('stage')
Outputs:
- output 1: float32 [], replicated
- output 2: float32 [12, 896, 4864], P('stage', 'data')
- output 3: float32 [12, 4864, 896], P('stage', None, 'data')
All inputs are finite; a program needn't handle non-finite values.
Results may differ from the reference program's by a relative error of at most 0.00938019.
Values are sent between devices in bfloat16 or wider.
A program may use at most 1 GiB of HBM per device.

```python
import jax
import jax.numpy as jnp
from jax import lax

WIDTH = 896
FFN = 4864
TOKENS = 64
MICRO = 4
REPLICAS = 8
LAYERS = 12

BATCH = REPLICAS * MICRO
TOTAL_TOKENS = BATCH * TOKENS


def setup_inputs(seed: int = 0) -> dict:
    base_key = jax.random.key(seed)
    key_in, key_tgt, key_up, key_down = jax.random.split(base_key, 4)
    inputs = jax.random.normal(key_in, (BATCH, TOKENS, WIDTH), jnp.float32).astype(jnp.bfloat16)
    targets = jax.random.normal(key_tgt, (BATCH, TOKENS, WIDTH), jnp.float32).astype(jnp.bfloat16)
    up_scale = WIDTH ** -0.5
    down_scale = 1.5 * (FFN * LAYERS) ** -0.5
    w_up = (jax.random.normal(key_up, (LAYERS, WIDTH, FFN), jnp.float32) * up_scale).astype(jnp.bfloat16)
    w_down = (jax.random.normal(key_down, (LAYERS, FFN, WIDTH), jnp.float32) * down_scale).astype(jnp.bfloat16)
    return {'inputs': inputs, 'targets': targets, 'w_up': w_up, 'w_down': w_down}


def layer_forward(h_in, w_one, w_two):
    pre_act = jnp.dot(h_in, w_one, preferred_element_type=jnp.float32).astype(jnp.bfloat16)
    act_out = jax.nn.gelu(pre_act.astype(jnp.float32)).astype(jnp.bfloat16)
    branch = jnp.dot(act_out, w_two, preferred_element_type=jnp.float32)
    return (h_in.astype(jnp.float32) + branch).astype(jnp.bfloat16)


def backward_inputs(h_in, grad_out, w_one, w_two):
    pre_act = jnp.dot(h_in, w_one, preferred_element_type=jnp.float32).astype(jnp.bfloat16)
    pre_wide = pre_act.astype(jnp.float32)
    act_out = jax.nn.gelu(pre_wide).astype(jnp.bfloat16)
    grad_act = jnp.dot(grad_out, w_two.T, preferred_element_type=jnp.float32).astype(jnp.bfloat16)
    grad_pre = jax.jvp(jax.nn.gelu, (pre_wide,), (grad_act.astype(jnp.float32),))[1].astype(jnp.bfloat16)
    grad_in = (grad_out.astype(jnp.float32) + jnp.dot(grad_pre, w_one.T, preferred_element_type=jnp.float32)).astype(jnp.bfloat16)
    return grad_in, act_out, grad_pre


def backward_weights(h_in, act_out, grad_pre, grad_out):
    grad_one = jnp.dot(h_in.T, grad_pre, preferred_element_type=jnp.float32)
    grad_two = jnp.dot(act_out.T, grad_out, preferred_element_type=jnp.float32)
    return grad_one, grad_two


def reference(inputs, targets, w_up, w_down):
    def fwd_step(hidden, weights):
        return layer_forward(hidden, weights[0], weights[1]), hidden

    def bwd_step(grad_out, layer_in):
        h_in, w_one, w_two = layer_in
        grad_in, act_out, grad_pre = backward_inputs(h_in, grad_out, w_one, w_two)
        return grad_in, backward_weights(h_in, act_out, grad_pre, grad_out)

    def micro_step(loop_state, batch_pair):
        up_acc, down_acc, loss_acc = loop_state
        x_mb, y_mb = batch_pair
        h_top, h_saved = lax.scan(fwd_step, x_mb, (w_up, w_down))
        out_diff = h_top.astype(jnp.float32) - y_mb.astype(jnp.float32)
        loss_mb = jnp.sum(out_diff * out_diff) / (2 * TOTAL_TOKENS)
        top_grad = (out_diff / TOTAL_TOKENS).astype(jnp.bfloat16)
        layer_grads = lax.scan(bwd_step, top_grad, (h_saved, w_up, w_down), reverse=True)[1]
        return (up_acc + layer_grads[0], down_acc + layer_grads[1], loss_acc + loss_mb), None

    init_state = (jnp.zeros(w_up.shape, jnp.float32), jnp.zeros(w_down.shape, jnp.float32), jnp.zeros((), jnp.float32))
    final_state = lax.scan(micro_step, init_state, (inputs, targets))[0]
    return final_state[2], final_state[0], final_state[1]
```

```python
import jax
import jax.numpy as jnp
from jax import lax
from jax.sharding import PartitionSpec as P

CONTRACT_LAST = (((1,), (1,)), ((), ()))
CONTRACT_FIRST = (((0,), (0,)), ((), ()))
SAME_CORE = [[0, 2, 4, 6], [1, 3, 5, 7]]
SWAP_CORE = [(0, 1), (1, 0), (2, 3), (3, 2), (4, 5), (5, 4), (6, 7), (7, 6)]


def up_proj(h_in, w_one):
    return jnp.dot(h_in, w_one, preferred_element_type=jnp.float32).astype(jnp.bfloat16)


def gelu_of(pre_act):
    return jax.nn.gelu(pre_act.astype(jnp.float32)).astype(jnp.bfloat16)


def grad_pre_of(grad_out, pre_act, w_two):
    grad_act = lax.dot_general(grad_out, w_two, CONTRACT_LAST, preferred_element_type=jnp.float32).astype(jnp.bfloat16)
    return jax.jvp(jax.nn.gelu, (pre_act.astype(jnp.float32),), (grad_act.astype(jnp.float32),))[1].astype(jnp.bfloat16)


def solution(mesh):
    stages = mesh.shape['stage']
    replicas = mesh.shape['data']
    fwd_perm = [(s, s + 1) for s in range(stages - 1)]
    bwd_perm = [(s + 1, s) for s in range(stages - 1)]

    def per_device(x_loc, y_loc, w_up, w_down):
        n_micro, n_tokens, n_width = x_loc.shape
        n_layers = w_up.shape[0]
        rows = n_micro * n_tokens
        total_tokens = replicas * rows
        stage_idx = lax.axis_index('stage')
        data_idx = lax.axis_index('data')
        x_rows = x_loc.reshape(rows, n_width)
        y_rows = y_loc.reshape(rows, n_width)
        zero_act = jnp.zeros((rows, n_width), jnp.bfloat16)

        hidden = x_rows
        h_saved = tuple(zero_act for _ in range(n_layers))
        u_saved = tuple(jnp.zeros((rows, w_up.shape[2]), jnp.bfloat16) for _ in range(n_layers))
        for tick in range(stages):
            def run_fwd(operands):
                h_cur, _, _ = operands
                hs, us = [], []
                for layer in range(n_layers):
                    hs.append(h_cur)
                    u = up_proj(h_cur, w_up[layer])
                    us.append(u)
                    branch = jnp.dot(gelu_of(u), w_down[layer], preferred_element_type=jnp.float32)
                    h_cur = (h_cur.astype(jnp.float32) + branch).astype(jnp.bfloat16)
                return h_cur, tuple(hs), tuple(us)

            hidden, h_saved, u_saved = lax.cond(stage_idx == tick, run_fwd, lambda ops: ops, (hidden, h_saved, u_saved))
            if tick < stages - 1:
                recv = lax.ppermute(hidden, 'stage', fwd_perm)
                hidden = jnp.where(stage_idx == tick + 1, recv, hidden)

        is_last = stage_idx == stages - 1
        out_diff = hidden.astype(jnp.float32) - y_rows.astype(jnp.float32)
        part_loss = jnp.where(is_last, jnp.sum(out_diff * out_diff) / (2 * total_tokens), 0.0)
        total_loss = lax.psum(part_loss, ('stage', 'data'))
        grad = (out_diff / total_tokens).astype(jnp.bfloat16)

        h_all = [lax.all_gather(h, 'data', axis_index_groups=SAME_CORE, tiled=True) for h in h_saved]

        e_saved = tuple(zero_act for _ in range(n_layers))
        for tick in reversed(range(stages)):
            def run_bwd(operands):
                e_cur, _ = operands
                es = [None] * n_layers
                for layer in reversed(range(n_layers)):
                    es[layer] = e_cur
                    du = grad_pre_of(e_cur, u_saved[layer], w_down[layer])
                    back = lax.dot_general(du, w_up[layer], CONTRACT_LAST, preferred_element_type=jnp.float32)
                    e_cur = (e_cur.astype(jnp.float32) + back).astype(jnp.bfloat16)
                return e_cur, tuple(es)

            grad, e_saved = lax.cond(stage_idx == tick, run_bwd, lambda ops: ops, (grad, e_saved))
            if tick > 0:
                recv = lax.ppermute(grad, 'stage', bwd_perm)
                grad = jnp.where(stage_idx == tick - 1, recv, grad)

        e_all = [lax.all_gather(e, 'data', axis_index_groups=SAME_CORE, tiled=True) for e in e_saved]

        chip = data_idx // 2
        core = data_idx % 2
        width_blk = n_width // replicas
        up_out, down_out = [], []
        for layer in range(n_layers):
            u = up_proj(h_all[layer], w_up[layer])
            g = gelu_of(u)
            du = grad_pre_of(e_all[layer], u, w_down[layer])
            h_cols = lax.dynamic_slice_in_dim(h_all[layer], chip * 2 * width_blk, 2 * width_blk, 1)
            e_cols = lax.dynamic_slice_in_dim(e_all[layer], chip * 2 * width_blk, 2 * width_blk, 1)
            g_one = lax.dot_general(h_cols, du, CONTRACT_FIRST, preferred_element_type=jnp.float32)
            g_two = lax.dot_general(g, e_cols, CONTRACT_FIRST, preferred_element_type=jnp.float32)
            send_one = lax.dynamic_slice_in_dim(g_one, (1 - core) * width_blk, width_blk, 0)
            keep_one = lax.dynamic_slice_in_dim(g_one, core * width_blk, width_blk, 0)
            send_two = lax.dynamic_slice_in_dim(g_two, (1 - core) * width_blk, width_blk, 1)
            keep_two = lax.dynamic_slice_in_dim(g_two, core * width_blk, width_blk, 1)
            up_out.append(keep_one + lax.ppermute(send_one, 'data', SWAP_CORE))
            down_out.append(keep_two + lax.ppermute(send_two, 'data', SWAP_CORE))
        return total_loss, jnp.stack(up_out), jnp.stack(down_out)

    return jax.shard_map(
        per_device,
        mesh=mesh,
        in_specs=(P('data', None, None), P('data', None, None), P('stage', None, None), P('stage', None, None)),
        out_specs=(P(), P('stage', 'data', None), P('stage', None, 'data')),
        check_vma=False,
    )
```

```python
import functools

import jax
import jax.numpy as jnp
from jax import lax
from jax.experimental import pallas as pl
from jax.experimental.pallas import tpu as pltpu
from jax.sharding import PartitionSpec as P

CONTRACT_LAST = (((1,), (1,)), ((), ()))
CONTRACT_FIRST = (((0,), (0,)), ((), ()))
SAME_CORE = [[0, 2, 4, 6], [1, 3, 5, 7]]
SWAP_CORE = [(0, 1), (1, 0), (2, 3), (3, 2), (4, 5), (5, 4), (6, 7), (7, 6)]
MESH = pl.DeviceIdType.MESH
GELU_C = 0.7978845608028654
GELU_A = 0.044715
CHIPS = 4


def up_proj(h_in, w_one):
    return jnp.dot(h_in, w_one, preferred_element_type=jnp.float32).astype(jnp.bfloat16)


def gelu_of(pre_act):
    return jax.nn.gelu(pre_act.astype(jnp.float32)).astype(jnp.bfloat16)


def grad_pre_of(grad_out, pre_act, w_two):
    grad_act = lax.dot_general(grad_out, w_two, CONTRACT_LAST, preferred_element_type=jnp.float32).astype(jnp.bfloat16)
    return jax.jvp(jax.nn.gelu, (pre_act.astype(jnp.float32),), (grad_act.astype(jnp.float32),))[1].astype(jnp.bfloat16)


def gelu_wide(u):
    th = jnp.tanh(u * (GELU_C + (GELU_C * GELU_A) * (u * u)))
    return u * (0.5 + 0.5 * th)


def gelu_slope(u):
    sq = u * u
    th = jnp.tanh(u * (GELU_C + (GELU_C * GELU_A) * sq))
    half = 0.5 + 0.5 * th
    return half + (0.5 * u) * (1.0 - th * th) * (GELU_C + (3.0 * GELU_C * GELU_A) * sq)


def chain_kernel(stages, total_tokens, x_ref, y_ref, w1_hbm, w2_hbm, h_all, e_out, loss_ref,
                 w1, w2, ut, g_buf, hs, e_t, e_nat, y_buf,
                 w1_sem, w2_sem, io_sem, hop_send, hop_recv, ag_send, ag_recv):
    stage = lax.axis_index('stage')
    data = lax.axis_index('data')
    chip = data // 2
    core = data % 2
    n_layers, width, ffn = w1.shape
    not_first = stage > 0
    not_last = stage < stages - 1

    def load_w1(l):
        return pltpu.make_async_copy(w1_hbm.at[l], w1.at[l], w1_sem.at[l])

    def load_w2(l, s):
        return pltpu.make_async_copy(w2_hbm.at[l], w2.at[l % 2], w2_sem.at[s])

    x_copy = pltpu.make_async_copy(x_ref, hs.at[0], io_sem.at[0])
    y_copy = pltpu.make_async_copy(y_ref, y_buf, io_sem.at[1])

    @pl.when(jnp.logical_not(not_first))
    def _():
        x_copy.start()

    load_w1(0).start()
    load_w2(0, 0).start()
    load_w1(1).start()
    load_w2(1, 1).start()
    load_w1(2).start()

    @pl.when(jnp.logical_not(not_last))
    def _():
        y_copy.start()

    peers = []
    for j in range(1, CHIPS):
        px = (chip // 2 + j // 2) % 2
        py = (chip % 2 + j % 2) % 2
        peers.append((px * 2 + py) * 2 + core)

    barrier = pltpu.get_barrier_semaphore()
    for p in peers:
        pl.semaphore_signal(barrier, inc=1, device_id=(stage, p), device_id_type=MESH)

    @pl.when(not_first)
    def _():
        pl.semaphore_signal(barrier, inc=1, device_id=(stage - 1, data), device_id_type=MESH)

    @pl.when(not_last)
    def _():
        pl.semaphore_signal(barrier, inc=1, device_id=(stage + 1, data), device_id_type=MESH)

    pl.semaphore_wait(barrier, CHIPS - 1 + jnp.minimum(stage, 1) + jnp.minimum(stages - 1 - stage, 1))

    def hop_up():
        return pltpu.make_async_remote_copy(
            src_ref=hs.at[n_layers], dst_ref=hs.at[0], send_sem=hop_send.at[0], recv_sem=hop_recv.at[0],
            device_id=(stage + 1, data), device_id_type=MESH)

    def hop_down():
        return pltpu.make_async_remote_copy(
            src_ref=e_t.at[0], dst_ref=e_t.at[n_layers], send_sem=hop_send.at[1], recv_sem=hop_recv.at[1],
            device_id=(stage - 1, data), device_id_type=MESH)

    def gather(l, j):
        return pltpu.make_async_remote_copy(
            src_ref=hs.at[l], dst_ref=h_all.at[l, chip], send_sem=ag_send.at[l, j], recv_sem=ag_recv.at[l, j],
            device_id=(stage, peers[j]), device_id_type=MESH)

    def keep(l):
        return pltpu.make_async_copy(hs.at[l], h_all.at[l, chip], io_sem.at[2 + l])

    @pl.when(not_first)
    def _():
        hop_up().wait_recv()

    @pl.when(jnp.logical_not(not_first))
    def _():
        x_copy.wait()

    def fwd_layer(l, carry):
        for j in range(CHIPS - 1):
            gather(l, j).start()
        keep(l).start()
        load_w1(l).wait()
        h = hs[l]
        for c in range(ffn // 256):
            cols = slice(c * 256, (c + 1) * 256)
            u = jnp.dot(h, w1[l, :, cols], preferred_element_type=jnp.float32).astype(jnp.bfloat16)
            ut[l, cols, :] = u.T
            g_buf[:, cols] = gelu_wide(u.astype(jnp.float32)).astype(jnp.bfloat16)
        load_w2(l, l).wait()
        branch = jnp.dot(g_buf[...], w2[l % 2], preferred_element_type=jnp.float32)
        hs[l + 1] = (h.astype(jnp.float32) + branch).astype(jnp.bfloat16)

        @pl.when(l == 0)
        def _():
            load_w2(2, 2).start()
        return carry

    lax.fori_loop(0, n_layers, fwd_layer, 0)

    @pl.when(not_last)
    def _():
        hop_up().start()
        loss_ref[...] = jnp.zeros_like(loss_ref)
        hop_up().wait_send()
        hop_down().wait_recv()

    @pl.when(jnp.logical_not(not_last))
    def _():
        y_copy.wait()
        diff = hs[n_layers].astype(jnp.float32) - y_buf[...].astype(jnp.float32)
        loss_ref[...] = jnp.sum(diff * diff, axis=0, keepdims=True)
        e_t[n_layers] = (diff / total_tokens).T.astype(jnp.bfloat16)

    rows_c = ffn // 4

    def bwd_layer(i, carry):
        l = n_layers - 1 - i

        @pl.when(l == 0)
        def _():
            load_w2(0, 3).wait()
        e_cur = e_t[l + 1]
        for c in range(4):
            rows = slice(c * rows_c, (c + 1) * rows_c)
            dg = jnp.dot(w2[l % 2, rows, :], e_cur, preferred_element_type=jnp.float32).astype(jnp.bfloat16)
            slope = gelu_slope(ut[l, rows, :].astype(jnp.float32))
            ut[l, rows, :] = (dg.astype(jnp.float32) * slope).astype(jnp.bfloat16)

        @pl.when(l == 2)
        def _():
            load_w2(0, 3).start()

        @pl.when(jnp.logical_or(not_first, l > 0))
        def _():
            back = jnp.dot(w1[l], ut[l], preferred_element_type=jnp.float32)
            e_t[l] = (e_cur.astype(jnp.float32) + back).astype(jnp.bfloat16)
        return carry

    lax.fori_loop(0, n_layers, bwd_layer, 0)

    @pl.when(not_first)
    def _():
        hop_down().start()

    for l in range(n_layers):
        e_nat[l] = e_t[l + 1].T
        pltpu.make_async_copy(e_nat.at[l], e_out.at[l], io_sem.at[5 + l]).start()
    for l in range(n_layers):
        pltpu.make_async_copy(e_nat.at[l], e_out.at[l], io_sem.at[5 + l]).wait()
        keep(l).wait()
        for j in range(CHIPS - 1):
            gather(l, j).wait_send()
            gather(l, j).wait_recv()

    @pl.when(not_first)
    def _():
        hop_down().wait_send()


def run_chain(x_rows, y_rows, w_up, w_down, stages, total_tokens):
    rows, width = x_rows.shape
    n_layers, _, ffn = w_up.shape
    bf = jnp.bfloat16
    any_spec = pl.BlockSpec(memory_space=pl.ANY)
    return pl.pallas_call(
        functools.partial(chain_kernel, stages, total_tokens),
        out_shape=(
            jax.ShapeDtypeStruct((n_layers, CHIPS, rows, width), bf),
            jax.ShapeDtypeStruct((n_layers, rows, width), bf),
            jax.ShapeDtypeStruct((1, width), jnp.float32),
        ),
        in_specs=[any_spec] * 4,
        out_specs=(any_spec, any_spec, pl.BlockSpec(memory_space=pltpu.VMEM)),
        scratch_shapes=[
            pltpu.VMEM((n_layers, width, ffn), bf),
            pltpu.VMEM((2, ffn, width), bf),
            pltpu.VMEM((n_layers, ffn, rows), bf),
            pltpu.VMEM((rows, ffn), bf),
            pltpu.VMEM((n_layers + 1, rows, width), bf),
            pltpu.VMEM((n_layers + 1, width, rows), bf),
            pltpu.VMEM((n_layers, rows, width), bf),
            pltpu.VMEM((rows, width), bf),
            pltpu.SemaphoreType.DMA((3,)),
            pltpu.SemaphoreType.DMA((4,)),
            pltpu.SemaphoreType.DMA((8,)),
            pltpu.SemaphoreType.DMA((2,)),
            pltpu.SemaphoreType.DMA((2,)),
            pltpu.SemaphoreType.DMA((3, 3)),
            pltpu.SemaphoreType.DMA((3, 3)),
        ],
        compiler_params=pltpu.CompilerParams(collective_id=0, has_side_effects=True, vmem_limit_bytes=67043328),
    )(x_rows, y_rows, w_up, w_down)


def solution(mesh):
    stages = mesh.shape['stage']
    replicas = mesh.shape['data']

    def per_device(x_loc, y_loc, w_up, w_down):
        n_micro, n_tokens, n_width = x_loc.shape
        n_layers = w_up.shape[0]
        rows = n_micro * n_tokens
        total_tokens = replicas * rows
        data_idx = lax.axis_index('data')
        x_rows = x_loc.reshape(rows, n_width)
        y_rows = y_loc.reshape(rows, n_width)
        h_gath, e_saved, loss_part = run_chain(x_rows, y_rows, w_up, w_down, stages, total_tokens)
        total_loss = lax.psum(jnp.sum(loss_part) / (2 * total_tokens), ('stage', 'data'))
        h_all = [h_gath[layer].reshape(CHIPS * rows, n_width) for layer in range(n_layers)]
        e_all = [lax.all_gather(e_saved[layer], 'data', axis_index_groups=SAME_CORE, tiled=True) for layer in range(n_layers)]

        chip = data_idx // 2
        core = data_idx % 2
        width_blk = n_width // replicas
        up_out, down_out = [], []
        for layer in range(n_layers):
            u = up_proj(h_all[layer], w_up[layer])
            g = gelu_of(u)
            du = grad_pre_of(e_all[layer], u, w_down[layer])
            h_cols = lax.dynamic_slice_in_dim(h_all[layer], chip * 2 * width_blk, 2 * width_blk, 1)
            e_cols = lax.dynamic_slice_in_dim(e_all[layer], chip * 2 * width_blk, 2 * width_blk, 1)
            g_one = lax.dot_general(h_cols, du, CONTRACT_FIRST, preferred_element_type=jnp.float32)
            g_two = lax.dot_general(g, e_cols, CONTRACT_FIRST, preferred_element_type=jnp.float32)
            send_one = lax.dynamic_slice_in_dim(g_one, (1 - core) * width_blk, width_blk, 0)
            keep_one = lax.dynamic_slice_in_dim(g_one, core * width_blk, width_blk, 0)
            send_two = lax.dynamic_slice_in_dim(g_two, (1 - core) * width_blk, width_blk, 1)
            keep_two = lax.dynamic_slice_in_dim(g_two, core * width_blk, width_blk, 1)
            up_out.append(keep_one + lax.ppermute(send_one, 'data', SWAP_CORE))
            down_out.append(keep_two + lax.ppermute(send_two, 'data', SWAP_CORE))
        return total_loss, jnp.stack(up_out), jnp.stack(down_out)

    return jax.shard_map(
        per_device,
        mesh=mesh,
        in_specs=(P('data', None, None), P('data', None, None), P('stage', None, None), P('stage', None, None)),
        out_specs=(P(), P('stage', 'data', None), P('stage', None, 'data')),
        check_vma=False,
    )
```

```python
import functools

import jax
import jax.numpy as jnp
from jax import lax
from jax.experimental import pallas as pl
from jax.experimental.pallas import tpu as pltpu
from jax.sharding import PartitionSpec as P

CONTRACT_LAST = (((1,), (1,)), ((), ()))
MESH = pl.DeviceIdType.MESH
GELU_C = 0.7978845608028654
GELU_A = 0.044715
CHIPS = 4


def gelu_wide(u):
    th = jnp.tanh(u * (GELU_C + (GELU_C * GELU_A) * (u * u)))
    return u * (0.5 + 0.5 * th)


def gelu_slope(u):
    sq = u * u
    th = jnp.tanh(u * (GELU_C + (GELU_C * GELU_A) * sq))
    half = 0.5 + 0.5 * th
    return half + (0.5 * u) * (1.0 - th * th) * (GELU_C + (3.0 * GELU_C * GELU_A) * sq)


def chain_kernel(stages, total_tokens, x_ref, y_ref, w1_hbm, w2_hbm, h_all, e_out, e_top, loss_ref,
                 w1, w2, ut, g_buf, hs, e_t, e_nat, y_buf, loss_buf, loss_tot,
                 w1_sem, w2_sem, io_sem, hop_send, hop_recv, ag_send, ag_recv, ls_send, ls_recv):
    stage = lax.axis_index('stage')
    data = lax.axis_index('data')
    chip = data // 2
    core = data % 2
    n_layers, width, ffn = w1.shape
    not_first = stage > 0
    not_last = stage < stages - 1

    def load_w1(l):
        return pltpu.make_async_copy(w1_hbm.at[l], w1.at[l], w1_sem.at[l])

    def load_w2(l, s):
        return pltpu.make_async_copy(w2_hbm.at[l], w2.at[l % 2], w2_sem.at[s])

    x_copy = pltpu.make_async_copy(x_ref, hs.at[0], io_sem.at[0])
    y_copy = pltpu.make_async_copy(y_ref, y_buf, io_sem.at[1])

    @pl.when(jnp.logical_not(not_first))
    def _():
        x_copy.start()

    load_w1(0).start()
    load_w2(0, 0).start()
    load_w1(1).start()
    load_w2(1, 1).start()
    load_w1(2).start()

    @pl.when(jnp.logical_not(not_last))
    def _():
        y_copy.start()

    peers = []
    for j in range(1, CHIPS):
        px = (chip // 2 + j // 2) % 2
        py = (chip % 2 + j % 2) % 2
        peers.append((px * 2 + py) * 2 + core)

    barrier = pltpu.get_barrier_semaphore()
    for k in range(1, 2 * CHIPS):
        pl.semaphore_signal(barrier, inc=1, device_id=(stage, (data + k) % (2 * CHIPS)), device_id_type=MESH)

    @pl.when(not_first)
    def _():
        pl.semaphore_signal(barrier, inc=1, device_id=(stage - 1, data), device_id_type=MESH)

    @pl.when(not_last)
    def _():
        pl.semaphore_signal(barrier, inc=1, device_id=(stage + 1, data), device_id_type=MESH)

    pl.semaphore_wait(barrier, 2 * CHIPS - 1 + jnp.minimum(stage, 1) + jnp.minimum(stages - 1 - stage, 1))

    def hop_up():
        return pltpu.make_async_remote_copy(
            src_ref=hs.at[n_layers], dst_ref=hs.at[0], send_sem=hop_send.at[0], recv_sem=hop_recv.at[0],
            device_id=(stage + 1, data), device_id_type=MESH)

    def hop_down():
        return pltpu.make_async_remote_copy(
            src_ref=e_t.at[0], dst_ref=e_t.at[n_layers], send_sem=hop_send.at[1], recv_sem=hop_recv.at[1],
            device_id=(stage - 1, data), device_id_type=MESH)

    def gather(l, j):
        return pltpu.make_async_remote_copy(
            src_ref=hs.at[l], dst_ref=h_all.at[l, chip], send_sem=ag_send.at[l, j], recv_sem=ag_recv.at[l, j],
            device_id=(stage, peers[j]), device_id_type=MESH)

    def keep(l):
        return pltpu.make_async_copy(hs.at[l], h_all.at[l, chip], io_sem.at[2 + l])

    top = n_layers - 1

    def gather_top(j):
        return pltpu.make_async_remote_copy(
            src_ref=e_nat.at[top], dst_ref=e_top.at[chip], send_sem=ag_send.at[n_layers, j],
            recv_sem=ag_recv.at[n_layers, j], device_id=(stage, peers[j]), device_id_type=MESH)

    def keep_e(l):
        dst = e_top.at[chip] if l == top else e_out.at[l]
        return pltpu.make_async_copy(e_nat.at[l], dst, io_sem.at[5 + l])

    def share_loss(k):
        return pltpu.make_async_remote_copy(
            src_ref=loss_buf.at[data], dst_ref=loss_buf.at[data], send_sem=ls_send.at[k - 1], recv_sem=ls_recv.at[k - 1],
            device_id=(stage, (data + k) % (2 * CHIPS)), device_id_type=MESH)

    def loss_down():
        return pltpu.make_async_remote_copy(
            src_ref=loss_tot, dst_ref=loss_tot, send_sem=hop_send.at[2], recv_sem=hop_recv.at[2],
            device_id=(stage - 1, data), device_id_type=MESH)

    @pl.when(not_first)
    def _():
        hop_up().wait_recv()

    @pl.when(jnp.logical_not(not_first))
    def _():
        x_copy.wait()

    def fwd_layer(l, carry):
        for j in range(CHIPS - 1):
            gather(l, j).start()
        keep(l).start()
        load_w1(l).wait()
        h = hs[l]
        for c in range(ffn // 256):
            cols = slice(c * 256, (c + 1) * 256)
            u = jnp.dot(h, w1[l, :, cols], preferred_element_type=jnp.float32).astype(jnp.bfloat16)
            ut[l, cols, :] = u.T
            g_buf[:, cols] = gelu_wide(u.astype(jnp.float32)).astype(jnp.bfloat16)
        load_w2(l, l).wait()
        branch = jnp.dot(g_buf[...], w2[l % 2], preferred_element_type=jnp.float32)
        hs[l + 1] = (h.astype(jnp.float32) + branch).astype(jnp.bfloat16)

        @pl.when(l == 0)
        def _():
            load_w2(2, 2).start()
        return carry

    lax.fori_loop(0, n_layers, fwd_layer, 0)

    @pl.when(not_last)
    def _():
        hop_up().start()
        hop_up().wait_send()
        hop_down().wait_recv()

    @pl.when(jnp.logical_not(not_last))
    def _():
        y_copy.wait()
        diff = hs[n_layers].astype(jnp.float32) - y_buf[...].astype(jnp.float32)
        e_t[n_layers] = (diff / total_tokens).T.astype(jnp.bfloat16)
        loss_buf[data] = jnp.full((8, 128), jnp.sum(diff * diff), jnp.float32)
        for k in range(1, 2 * CHIPS):
            share_loss(k).start()

    rows_c = ffn // 4

    def bwd_layer(i, carry):
        l = n_layers - 1 - i

        @pl.when(l == 0)
        def _():
            load_w2(0, 3).wait()
        e_cur = e_t[l + 1]
        e_nat[l] = e_cur.T
        for c in range(4):
            rows = slice(c * rows_c, (c + 1) * rows_c)
            dg = jnp.dot(w2[l % 2, rows, :], e_cur, preferred_element_type=jnp.float32).astype(jnp.bfloat16)
            slope = gelu_slope(ut[l, rows, :].astype(jnp.float32))
            ut[l, rows, :] = (dg.astype(jnp.float32) * slope).astype(jnp.bfloat16)

        @pl.when(l == 2)
        def _():
            load_w2(0, 3).start()
            for j in range(CHIPS - 1):
                gather_top(j).start()
            keep_e(top).start()

        @pl.when(jnp.logical_or(not_first, l > 0))
        def _():
            back = jnp.dot(w1[l], ut[l], preferred_element_type=jnp.float32)
            e_t[l] = (e_cur.astype(jnp.float32) + back).astype(jnp.bfloat16)
        return carry

    lax.fori_loop(0, n_layers, bwd_layer, 0)

    @pl.when(not_first)
    def _():
        hop_down().start()

    for l in range(top):
        keep_e(l).start()

    @pl.when(not_last)
    def _():
        loss_down().wait_recv()

    @pl.when(jnp.logical_not(not_last))
    def _():
        for k in range(1, 2 * CHIPS):
            share_loss(k).wait_send()
            share_loss(k).wait_recv()
        total = loss_buf[0]
        for k in range(1, 2 * CHIPS):
            total = total + loss_buf[k]
        loss_tot[...] = total / (2 * total_tokens)

    loss_ref[...] = loss_tot[...]

    @pl.when(not_first)
    def _():
        loss_down().start()

    for l in range(n_layers):
        keep_e(l).wait()
        keep(l).wait()
        for j in range(CHIPS - 1):
            gather(l, j).wait_send()
            gather(l, j).wait_recv()
    for j in range(CHIPS - 1):
        gather_top(j).wait_send()
        gather_top(j).wait_recv()

    @pl.when(not_first)
    def _():
        hop_down().wait_send()
        loss_down().wait_send()


def run_chain(x_rows, y_rows, w_up, w_down, stages, total_tokens):
    rows, width = x_rows.shape
    n_layers, _, ffn = w_up.shape
    bf = jnp.bfloat16
    any_spec = pl.BlockSpec(memory_space=pl.ANY)
    return pl.pallas_call(
        functools.partial(chain_kernel, stages, total_tokens),
        out_shape=(
            jax.ShapeDtypeStruct((n_layers, CHIPS, rows, width), bf),
            jax.ShapeDtypeStruct((n_layers - 1, rows, width), bf),
            jax.ShapeDtypeStruct((CHIPS, rows, width), bf),
            jax.ShapeDtypeStruct((8, 128), jnp.float32),
        ),
        in_specs=[any_spec] * 4,
        out_specs=(any_spec, any_spec, any_spec, pl.BlockSpec(memory_space=pltpu.VMEM)),
        scratch_shapes=[
            pltpu.VMEM((n_layers, width, ffn), bf),
            pltpu.VMEM((2, ffn, width), bf),
            pltpu.VMEM((n_layers, ffn, rows), bf),
            pltpu.VMEM((rows, ffn), bf),
            pltpu.VMEM((n_layers + 1, rows, width), bf),
            pltpu.VMEM((n_layers + 1, width, rows), bf),
            pltpu.VMEM((n_layers, rows, width), bf),
            pltpu.VMEM((rows, width), bf),
            pltpu.VMEM((2 * CHIPS, 8, 128), jnp.float32),
            pltpu.VMEM((8, 128), jnp.float32),
            pltpu.SemaphoreType.DMA((3,)),
            pltpu.SemaphoreType.DMA((4,)),
            pltpu.SemaphoreType.DMA((8,)),
            pltpu.SemaphoreType.DMA((3,)),
            pltpu.SemaphoreType.DMA((3,)),
            pltpu.SemaphoreType.DMA((4, 3)),
            pltpu.SemaphoreType.DMA((4, 3)),
            pltpu.SemaphoreType.DMA((7,)),
            pltpu.SemaphoreType.DMA((7,)),
        ],
        compiler_params=pltpu.CompilerParams(collective_id=0, has_side_effects=True, vmem_limit_bytes=67043328),
    )(x_rows, y_rows, w_up, w_down)


CHUNK = 256
RING = 4


def weight_kernel(h_hbm, e_own, e_top, w1_hbm, w2_hbm, out1, out2,
                  h_buf, e_buf, w1s, w2s, hct, ect, u_a, dg_a, u_b, dg_b, part, recv, turn,
                  w_sem, h_sem, e_sem, o_sem, ag_send, ag_recv, x_send, x_recv):
    stage = lax.axis_index('stage')
    data = lax.axis_index('data')
    chip = data // 2
    core = data % 2
    n_layers, width, ffn = w1_hbm.shape
    n_chunks = ffn // CHUNK
    total = n_layers * n_chunks
    blk = out1.shape[1]
    rows = e_own.shape[1]
    top = n_layers - 1
    partner = data + 1 - 2 * core

    def load_w(q):
        qq = jnp.minimum(q, total - 1)
        l = top - qq // n_chunks
        cols = pl.ds(pl.multiple_of((qq % n_chunks) * CHUNK, CHUNK), CHUNK)
        s = q % RING
        return (pltpu.make_async_copy(w1_hbm.at[l, :, cols], w1s.at[s], w_sem.at[0, s]),
                pltpu.make_async_copy(w2_hbm.at[l, cols, :], w2s.at[s], w_sem.at[1, s]))

    def load_h(l):
        return pltpu.make_async_copy(h_hbm.at[l], h_buf.at[l], h_sem.at[l])

    load_h(top).start()
    top_copy = pltpu.make_async_copy(e_top, e_buf.at[top], e_sem.at[top])
    top_copy.start()
    for q in range(RING - 1):
        for cp in load_w(q):
            cp.start()

    peers = []
    for j in range(1, CHIPS):
        px = (chip // 2 + j // 2) % 2
        py = (chip % 2 + j % 2) % 2
        peers.append((px * 2 + py) * 2 + core)
    barrier = pltpu.get_barrier_semaphore()
    for p in peers + [partner]:
        pl.semaphore_signal(barrier, inc=1, device_id=(stage, p), device_id_type=MESH)
    pl.semaphore_wait(barrier, CHIPS)

    def gather(l, j):
        return pltpu.make_async_remote_copy(
            src_ref=e_own.at[l], dst_ref=e_buf.at[l, chip], send_sem=ag_send.at[l, j], recv_sem=ag_recv.at[l, j],
            device_id=(stage, peers[j]), device_id_type=MESH)

    def keep(l):
        return pltpu.make_async_copy(e_own.at[l], e_buf.at[l, chip], e_sem.at[l])

    for l in reversed(range(top)):
        for j in range(CHIPS - 1):
            gather(l, j).start()
        keep(l).start()
        load_h(l).start()

    def swap(l, par, k):
        return pltpu.make_async_remote_copy(
            src_ref=part.at[par, k, 1 - core], dst_ref=recv.at[l, k], send_sem=x_send.at[l, k], recv_sem=x_recv.at[l, k],
            device_id=(stage, partner), device_id_type=MESH)

    def put_one(l, par):
        return pltpu.make_async_copy(part.at[par, 0, core], out1.at[l], o_sem.at[0])

    def put_two(l):
        return pltpu.make_async_copy(turn, out2.at[l], o_sem.at[1])

    def finish(l, par):
        for k in range(2):
            swap(l, par, k).wait_send()
            swap(l, par, k).wait_recv()

        def add(c, carry):
            cols = pl.ds(pl.multiple_of(c * CHUNK, CHUNK), CHUNK)
            part[par, 0, core, :, cols] = part[par, 0, core, :, cols] + recv[l, 0, :, cols]
            both = part[par, 1, core, :, cols] + recv[l, 1, :, cols]
            turn[cols, :] = both.T
            return carry

        lax.fori_loop(0, n_chunks, add, 0)
        put_one(l, par).start()
        put_two(l).start()
        put_one(l, par).wait()
        put_two(l).wait()

    def layer_step(li, carry):
        l = top - li
        par = li % 2
        load_h(l).wait()

        @pl.when(li == 0)
        def _():
            top_copy.wait()

        @pl.when(li > 0)
        def _():
            keep(l).wait()
            for j in range(CHIPS - 1):
                gather(l, j).wait_recv()

        n_rows = CHIPS * rows
        for k in range(CHIPS):
            @pl.when(chip == k)
            def _():
                lanes = slice(k * 2 * blk, (k + 1) * 2 * blk)
                for r in range(CHIPS):
                    hct[:, r * rows:(r + 1) * rows] = h_buf[l, r, :, lanes].T
                    ect[:, r * rows:(r + 1) * rows] = e_buf[l, r, :, lanes].T

        def mm(c, u_ref, dg_ref):
            q = li * n_chunks + c
            for cp in load_w(q):
                cp.wait()
            for cp in load_w(q + RING - 1):
                cp.start()
            s = q % RING
            h = h_buf[l].reshape(n_rows, width)
            e = e_buf[l].reshape(n_rows, width)
            u_ref[...] = jnp.dot(h, w1s[s], preferred_element_type=jnp.float32).astype(jnp.bfloat16)
            dg_ref[...] = lax.dot_general(e, w2s[s], CONTRACT_LAST, preferred_element_type=jnp.float32).astype(jnp.bfloat16)

        def ew(c, u_ref, dg_ref):
            cols = pl.ds(pl.multiple_of(c * CHUNK, CHUNK), CHUNK)
            u = u_ref[...].astype(jnp.float32)
            sq = u * u
            half = 0.5 + 0.5 * jnp.tanh(u * (GELU_C + (GELU_C * GELU_A) * sq))
            g = (u * half).astype(jnp.bfloat16)
            slope = half + (half - half * half) * (u * (2.0 * GELU_C + (6.0 * GELU_C * GELU_A) * sq))
            du = (dg_ref[...].astype(jnp.float32) * slope).astype(jnp.bfloat16)
            d1 = jnp.dot(hct[...], du, preferred_element_type=jnp.float32)
            d2 = jnp.dot(ect[...], g, preferred_element_type=jnp.float32)
            for k in range(2):
                part[par, 0, k, :, cols] = d1[k * blk:(k + 1) * blk]
                part[par, 1, k, :, cols] = d2[k * blk:(k + 1) * blk]

        mm(0, u_a, dg_a)

        def pair(i, c2):
            mm(2 * i + 1, u_b, dg_b)
            ew(2 * i, u_a, dg_a)
            mm(2 * i + 2, u_a, dg_a)
            ew(2 * i + 1, u_b, dg_b)
            return c2

        lax.fori_loop(0, n_chunks // 2, pair, 0)
        ew(n_chunks - 1, u_a, dg_a)
        for k in range(2):
            swap(l, par, k).start()

        @pl.when(li > 0)
        def _():
            finish(l + 1, (li + 1) % 2)
        return carry

    lax.fori_loop(0, n_layers, layer_step, 0)
    finish(0, top % 2)
    for q in range(total, total + RING - 1):
        for cp in load_w(q):
            cp.wait()
    for l in range(top):
        for j in range(CHIPS - 1):
            gather(l, j).wait_send()


def run_weights(h_gath, e_own, e_top, w_up, w_down):
    n_layers, _, rows, width = h_gath.shape
    ffn = w_up.shape[2]
    blk = width // (2 * CHIPS)
    bf, f32 = jnp.bfloat16, jnp.float32
    any_spec = pl.BlockSpec(memory_space=pl.ANY)
    dma = pltpu.SemaphoreType.DMA
    return pl.pallas_call(
        weight_kernel,
        out_shape=(
            jax.ShapeDtypeStruct((n_layers, blk, ffn), f32),
            jax.ShapeDtypeStruct((n_layers, ffn, blk), f32),
        ),
        in_specs=[any_spec] * 5,
        out_specs=(any_spec, any_spec),
        scratch_shapes=[
            pltpu.VMEM((n_layers, CHIPS, rows, width), bf),
            pltpu.VMEM((n_layers, CHIPS, rows, width), bf),
            pltpu.VMEM((RING, width, CHUNK), bf),
            pltpu.VMEM((RING, CHUNK, width), bf),
            pltpu.VMEM((2 * blk, CHIPS * rows), bf),
            pltpu.VMEM((2 * blk, CHIPS * rows), bf),
            pltpu.VMEM((CHIPS * rows, CHUNK), bf),
            pltpu.VMEM((CHIPS * rows, CHUNK), bf),
            pltpu.VMEM((CHIPS * rows, CHUNK), bf),
            pltpu.VMEM((CHIPS * rows, CHUNK), bf),
            pltpu.VMEM((2, 2, 2, blk, ffn), f32),
            pltpu.VMEM((n_layers, 2, blk, ffn), f32),
            pltpu.VMEM((ffn, blk), f32),
            dma((2, RING)), dma((3,)), dma((3,)), dma((2,)),
            dma((2, 3)), dma((2, 3)), dma((3, 2)), dma((3, 2)),
        ],
        compiler_params=pltpu.CompilerParams(collective_id=1, has_side_effects=True, vmem_limit_bytes=67043328),
    )(h_gath, e_own, e_top, w_up, w_down)


def solution(mesh):
    stages = mesh.shape['stage']
    replicas = mesh.shape['data']

    def per_device(x_loc, y_loc, w_up, w_down):
        n_micro, n_tokens, n_width = x_loc.shape
        n_layers = w_up.shape[0]
        rows = n_micro * n_tokens
        total_tokens = replicas * rows
        x_rows = x_loc.reshape(rows, n_width)
        y_rows = y_loc.reshape(rows, n_width)
        h_gath, e_own, e_top, loss = run_chain(x_rows, y_rows, w_up, w_down, stages, total_tokens)
        grad_up, grad_down = run_weights(h_gath, e_own, e_top, w_up, w_down)
        return loss[0, 0], grad_up, grad_down

    return jax.shard_map(
        per_device,
        mesh=mesh,
        in_specs=(P('data', None, None), P('data', None, None), P('stage', None, None), P('stage', None, None)),
        out_specs=(P(), P('stage', 'data', None), P('stage', None, 'data')),
        check_vma=False,
    )
```

```python
import functools

import jax
import jax.numpy as jnp
from jax import lax
from jax.experimental import pallas as pl
from jax.experimental.pallas import tpu as pltpu
from jax.sharding import PartitionSpec as P

CONTRACT_LAST = (((1,), (1,)), ((), ()))
MESH = pl.DeviceIdType.MESH
GELU_C = 0.7978845608028654
GELU_A = 0.044715
CHIPS = 4


def gelu_wide(u):
    th = jnp.tanh(u * (GELU_C + (GELU_C * GELU_A) * (u * u)))
    return u * (0.5 + 0.5 * th)


def gelu_slope(u):
    sq = u * u
    th = jnp.tanh(u * (GELU_C + (GELU_C * GELU_A) * sq))
    half = 0.5 + 0.5 * th
    return half + (0.5 * u) * (1.0 - th * th) * (GELU_C + (3.0 * GELU_C * GELU_A) * sq)


def chain_kernel(stages, total_tokens, x_ref, y_ref, w1_hbm, w2_hbm, h_all, e_out, e_top, loss_ref,
                 w1, w2, ut, g_buf, hs, e_t, e_nat, y_buf, loss_buf, loss_tot,
                 w1_sem, w2_sem, io_sem, hop_send, hop_recv, ag_send, ag_recv, ls_send, ls_recv, turn_sem):
    stage = lax.axis_index('stage')
    data = lax.axis_index('data')
    chip = data // 2
    core = data % 2
    n_layers, width, ffn = w1.shape
    not_first = stage > 0
    not_last = stage < stages - 1
    is_first = jnp.logical_not(not_first)
    is_last = jnp.logical_not(not_last)
    pieces = ((0, 512), (512, width))

    def load_w1(l):
        return pltpu.make_async_copy(w1_hbm.at[l], w1.at[l], w1_sem.at[l])

    def load_w2(l, s):
        return pltpu.make_async_copy(w2_hbm.at[l], w2.at[l % 2], w2_sem.at[s])

    x_copy = pltpu.make_async_copy(x_ref, hs.at[0], io_sem.at[0])
    y_copy = pltpu.make_async_copy(y_ref, y_buf, io_sem.at[1])

    @pl.when(jnp.logical_not(not_first))
    def _():
        x_copy.start()

    load_w1(0).start()

    @pl.when(not_first)
    def _():
        load_w2(0, 0).start()
        load_w1(1).start()
        load_w2(1, 1).start()
        load_w1(2).start()

    @pl.when(jnp.logical_not(not_last))
    def _():
        y_copy.start()

    peers = []
    for j in range(1, CHIPS):
        px = (chip // 2 + j // 2) % 2
        py = (chip % 2 + j % 2) % 2
        peers.append((px * 2 + py) * 2 + core)

    barrier = pltpu.get_barrier_semaphore()
    for k in range(1, 2 * CHIPS):
        pl.semaphore_signal(barrier, inc=1, device_id=(stage, (data + k) % (2 * CHIPS)), device_id_type=MESH)

    @pl.when(not_first)
    def _():
        pl.semaphore_signal(barrier, inc=1, device_id=(stage - 1, data), device_id_type=MESH)

    @pl.when(not_last)
    def _():
        pl.semaphore_signal(barrier, inc=1, device_id=(stage + 1, data), device_id_type=MESH)

    pl.semaphore_wait(barrier, 2 * CHIPS - 1 + jnp.minimum(stage, 1) + jnp.minimum(stages - 1 - stage, 1))

    def hop_up(p):
        lanes = slice(*pieces[p])
        return pltpu.make_async_remote_copy(
            src_ref=hs.at[n_layers, :, lanes], dst_ref=hs.at[0, :, lanes], send_sem=hop_send.at[0, p],
            recv_sem=hop_recv.at[0, p], device_id=(stage + 1, data), device_id_type=MESH)

    def hop_down(p):
        subl = slice(*pieces[p])
        return pltpu.make_async_remote_copy(
            src_ref=e_t.at[0, subl, :], dst_ref=e_t.at[n_layers, subl, :], send_sem=hop_send.at[1, p],
            recv_sem=hop_recv.at[1, p], device_id=(stage - 1, data), device_id_type=MESH)

    def gather(l, j):
        return pltpu.make_async_remote_copy(
            src_ref=hs.at[l], dst_ref=h_all.at[l, chip], send_sem=ag_send.at[l, j], recv_sem=ag_recv.at[l, j],
            device_id=(stage, peers[j]), device_id_type=MESH)

    def keep(l):
        return pltpu.make_async_copy(hs.at[l], h_all.at[l, chip], io_sem.at[2 + l])

    top = n_layers - 1

    def gather_top(j):
        return pltpu.make_async_remote_copy(
            src_ref=e_nat.at[top], dst_ref=e_top.at[chip], send_sem=ag_send.at[n_layers, j],
            recv_sem=ag_recv.at[n_layers, j], device_id=(stage, peers[j]), device_id_type=MESH)

    def keep_e(l):
        dst = e_top.at[chip] if l == top else e_out.at[l]
        return pltpu.make_async_copy(e_nat.at[l], dst, io_sem.at[5 + l])

    def share_loss(k):
        return pltpu.make_async_remote_copy(
            src_ref=loss_buf.at[data], dst_ref=loss_buf.at[data], send_sem=ls_send.at[k - 1], recv_sem=ls_recv.at[k - 1],
            device_id=(stage, (data + k) % (2 * CHIPS)), device_id_type=MESH)

    def loss_down():
        return pltpu.make_async_remote_copy(
            src_ref=loss_tot, dst_ref=loss_tot, send_sem=hop_send.at[2, 0], recv_sem=hop_recv.at[2, 0],
            device_id=(stage - 1, data), device_id_type=MESH)

    @pl.when(not_first)
    def _():
        hop_up(0).wait_recv()
        hop_up(1).wait_recv()

    @pl.when(is_first)
    def _():
        x_copy.wait()

    send_now = jnp.logical_and(not_last, jnp.logical_or(not_first, core == 0))

    def fwd_layer(l, carry):
        for j in range(CHIPS - 1):
            gather(l, j).start()
        keep(l).start()
        load_w1(l).wait()

        @pl.when(is_first)
        def _():
            @pl.when(l < top)
            def _():
                load_w2(l, l).start()
        h = hs[l]
        for c in range(ffn // 256):
            cols = slice(c * 256, (c + 1) * 256)
            u = jnp.dot(h, w1[l, :, cols], preferred_element_type=jnp.float32).astype(jnp.bfloat16)
            ut[l, cols, :] = u.T
            g_buf[:, cols] = gelu_wide(u.astype(jnp.float32)).astype(jnp.bfloat16)
        load_w2(l, l).wait()

        @pl.when(is_first)
        def _():
            @pl.when(l < top)
            def _():
                load_w1(l + 1).start()
        for p in range(2):
            lanes = slice(*pieces[p])
            branch = jnp.dot(g_buf[...], w2[l % 2, :, lanes], preferred_element_type=jnp.float32)
            hs[l + 1, :, lanes] = (hs[l, :, lanes].astype(jnp.float32) + branch).astype(jnp.bfloat16)

            @pl.when(jnp.logical_and(l == top, send_now))
            def _():
                hop_up(p).start()

        @pl.when(l == 0)
        def _():
            load_w2(2, 2).start()
        return carry

    lax.fori_loop(0, n_layers, fwd_layer, 0)

    @pl.when(jnp.logical_and(is_first, core == 1))
    def _():
        pl.semaphore_wait(turn_sem, 1)
        hop_up(0).start()
        hop_up(1).start()

    @pl.when(not_last)
    def _():
        hop_up(0).wait_send()
        hop_up(1).wait_send()

    @pl.when(jnp.logical_and(is_first, core == 0))
    def _():
        pl.semaphore_signal(turn_sem, inc=1, device_id=(stage, data + 1), device_id_type=MESH)

    @pl.when(not_last)
    def _():
        hop_down(0).wait_recv()
        hop_down(1).wait_recv()

    @pl.when(is_last)
    def _():
        y_copy.wait()
        diff = hs[n_layers].astype(jnp.float32) - y_buf[...].astype(jnp.float32)
        e_t[n_layers] = (diff / total_tokens).T.astype(jnp.bfloat16)
        loss_buf[data] = jnp.full((8, 128), jnp.sum(diff * diff), jnp.float32)
        for k in range(1, 2 * CHIPS):
            share_loss(k).start()

    e_nat[top] = e_t[n_layers].T
    for j in range(CHIPS - 1):
        gather_top(j).start()
    keep_e(top).start()
    rows_c = ffn // 19

    def bwd_layer(i, carry):
        l = n_layers - 1 - i

        @pl.when(l == 0)
        def _():
            load_w2(0, 3).wait()
        e_cur = e_t[l + 1]

        @pl.when(l < top)
        def _():
            e_nat[l] = e_t[l + 1].T
        for c in range(19):
            rows = slice(c * rows_c, (c + 1) * rows_c)
            dg = jnp.dot(w2[l % 2, rows, :], e_cur, preferred_element_type=jnp.float32).astype(jnp.bfloat16)
            slope = gelu_slope(ut[l, rows, :].astype(jnp.float32))
            ut[l, rows, :] = (dg.astype(jnp.float32) * slope).astype(jnp.bfloat16)

        @pl.when(l == 2)
        def _():
            load_w2(0, 3).start()

        @pl.when(jnp.logical_or(not_first, l > 0))
        def _():
            for p in range(2):
                subl = slice(*pieces[p])
                back = jnp.dot(w1[l, subl, :], ut[l], preferred_element_type=jnp.float32)
                e_t[l, subl, :] = (e_t[l + 1, subl, :].astype(jnp.float32) + back).astype(jnp.bfloat16)

                @pl.when(l == 0)
                def _():
                    hop_down(p).start()
        return carry

    lax.fori_loop(0, n_layers, bwd_layer, 0)

    for l in range(top):
        keep_e(l).start()

    @pl.when(not_last)
    def _():
        loss_down().wait_recv()

    @pl.when(is_last)
    def _():
        for k in range(1, 2 * CHIPS):
            share_loss(k).wait_send()
            share_loss(k).wait_recv()
        total = loss_buf[0]
        for k in range(1, 2 * CHIPS):
            total = total + loss_buf[k]
        loss_tot[...] = total / (2 * total_tokens)

    loss_ref[...] = loss_tot[...]

    @pl.when(not_first)
    def _():
        loss_down().start()

    for l in range(n_layers):
        keep_e(l).wait()
        keep(l).wait()
        for j in range(CHIPS - 1):
            gather(l, j).wait_send()
            gather(l, j).wait_recv()
    for j in range(CHIPS - 1):
        gather_top(j).wait_send()
        gather_top(j).wait_recv()

    @pl.when(not_first)
    def _():
        hop_down(0).wait_send()
        hop_down(1).wait_send()
        loss_down().wait_send()


def run_chain(x_rows, y_rows, w_up, w_down, stages, total_tokens):
    rows, width = x_rows.shape
    n_layers, _, ffn = w_up.shape
    bf = jnp.bfloat16
    any_spec = pl.BlockSpec(memory_space=pl.ANY)
    return pl.pallas_call(
        functools.partial(chain_kernel, stages, total_tokens),
        out_shape=(
            jax.ShapeDtypeStruct((n_layers, CHIPS, rows, width), bf),
            jax.ShapeDtypeStruct((n_layers - 1, rows, width), bf),
            jax.ShapeDtypeStruct((CHIPS, rows, width), bf),
            jax.ShapeDtypeStruct((8, 128), jnp.float32),
        ),
        in_specs=[any_spec] * 4,
        out_specs=(any_spec, any_spec, any_spec, pl.BlockSpec(memory_space=pltpu.VMEM)),
        scratch_shapes=[
            pltpu.VMEM((n_layers, width, ffn), bf),
            pltpu.VMEM((2, ffn, width), bf),
            pltpu.VMEM((n_layers, ffn, rows), bf),
            pltpu.VMEM((rows, ffn), bf),
            pltpu.VMEM((n_layers + 1, rows, width), bf),
            pltpu.VMEM((n_layers + 1, width, rows), bf),
            pltpu.VMEM((n_layers, rows, width), bf),
            pltpu.VMEM((rows, width), bf),
            pltpu.VMEM((2 * CHIPS, 8, 128), jnp.float32),
            pltpu.VMEM((8, 128), jnp.float32),
            pltpu.SemaphoreType.DMA((3,)),
            pltpu.SemaphoreType.DMA((4,)),
            pltpu.SemaphoreType.DMA((8,)),
            pltpu.SemaphoreType.DMA((3, 2)),
            pltpu.SemaphoreType.DMA((3, 2)),
            pltpu.SemaphoreType.DMA((4, 3)),
            pltpu.SemaphoreType.DMA((4, 3)),
            pltpu.SemaphoreType.DMA((7,)),
            pltpu.SemaphoreType.DMA((7,)),
            pltpu.SemaphoreType.REGULAR,
        ],
        compiler_params=pltpu.CompilerParams(collective_id=0, has_side_effects=True, vmem_limit_bytes=67043328),
    )(x_rows, y_rows, w_up, w_down)


CHUNK = 256
RING = 4


def weight_kernel(h_hbm, e_own, e_top, w1_hbm, w2_hbm, out1, out2,
                  h_buf, e_buf, w1s, w2s, hct, ect, u_a, dg_a, u_b, dg_b, part, recv, turn,
                  w_sem, h_sem, e_sem, o_sem, ag_send, ag_recv, x_send, x_recv):
    stage = lax.axis_index('stage')
    data = lax.axis_index('data')
    chip = data // 2
    core = data % 2
    n_layers, width, ffn = w1_hbm.shape
    n_chunks = ffn // CHUNK
    total = n_layers * n_chunks
    blk = out1.shape[1]
    rows = e_own.shape[1]
    top = n_layers - 1
    partner = data + 1 - 2 * core

    def load_w(q):
        qq = jnp.minimum(q, total - 1)
        l = top - qq // n_chunks
        cols = pl.ds(pl.multiple_of((qq % n_chunks) * CHUNK, CHUNK), CHUNK)
        s = q % RING
        return (pltpu.make_async_copy(w1_hbm.at[l, :, cols], w1s.at[s], w_sem.at[0, s]),
                pltpu.make_async_copy(w2_hbm.at[l, cols, :], w2s.at[s], w_sem.at[1, s]))

    def load_h(l):
        return pltpu.make_async_copy(h_hbm.at[l], h_buf.at[l], h_sem.at[l])

    load_h(top).start()
    top_copy = pltpu.make_async_copy(e_top, e_buf.at[top], e_sem.at[top])
    top_copy.start()
    for q in range(2):
        for cp in load_w(q):
            cp.start()

    peers = []
    for j in range(1, CHIPS):
        px = (chip // 2 + j // 2) % 2
        py = (chip % 2 + j % 2) % 2
        peers.append((px * 2 + py) * 2 + core)
    barrier = pltpu.get_barrier_semaphore()
    for p in peers + [partner]:
        pl.semaphore_signal(barrier, inc=1, device_id=(stage, p), device_id_type=MESH)
    pl.semaphore_wait(barrier, CHIPS)

    def gather(l, j):
        return pltpu.make_async_remote_copy(
            src_ref=e_own.at[l], dst_ref=e_buf.at[l, chip], send_sem=ag_send.at[l, j], recv_sem=ag_recv.at[l, j],
            device_id=(stage, peers[j]), device_id_type=MESH)

    def keep(l):
        return pltpu.make_async_copy(e_own.at[l], e_buf.at[l, chip], e_sem.at[l])

    for l in reversed(range(top)):
        for j in range(CHIPS - 1):
            gather(l, j).start()
        keep(l).start()
        load_h(l).start()

    half_chunks = n_chunks // 2 + 1
    groups = (slice(0, half_chunks * CHUNK), slice(half_chunks * CHUNK, ffn))

    def swap(l, k, p):
        return pltpu.make_async_remote_copy(
            src_ref=part.at[l, k, 1 - core, :, groups[p]], dst_ref=recv.at[l, k, :, groups[p]],
            send_sem=x_send.at[l, k, p], recv_sem=x_recv.at[l, k, p],
            device_id=(stage, partner), device_id_type=MESH)

    def put(l):
        return (pltpu.make_async_copy(part.at[l, 0, core], out1.at[l], o_sem.at[0, l]),
                pltpu.make_async_copy(turn.at[l % 2], out2.at[l], o_sem.at[1, l]))

    def finish(l, c):
        cols = pl.ds(pl.multiple_of(c * CHUNK, CHUNK), CHUNK)
        part[l, 0, core, :, cols] = part[l, 0, core, :, cols] + recv[l, 0, :, cols]
        both = part[l, 1, core, :, cols] + recv[l, 1, :, cols]
        turn[l % 2, cols, :] = both.T

    def swap_start(l, p):
        for k in range(2):
            swap(l, k, p).start()

    def swap_wait(l, p):
        for k in range(2):
            swap(l, k, p).wait_send()
            swap(l, k, p).wait_recv()

    def layer_step(li, first):
        l = top - li
        load_h(l).wait()
        if first:
            top_copy.wait()
        else:
            keep(l).wait()
            for j in range(CHIPS - 1):
                gather(l, j).wait_recv()

        n_rows = CHIPS * rows
        for k in range(CHIPS):
            @pl.when(chip == k)
            def _():
                lanes = slice(k * 2 * blk, (k + 1) * 2 * blk)
                for r in range(CHIPS):
                    hct[:, r * rows:(r + 1) * rows] = h_buf[l, r, :, lanes].T
                    ect[:, r * rows:(r + 1) * rows] = e_buf[l, r, :, lanes].T

        def mm(c, u_ref, dg_ref):
            q = li * n_chunks + c
            s = q % RING
            h = h_buf[l].reshape(n_rows, width)
            e = e_buf[l].reshape(n_rows, width)
            u_ref[...] = jnp.dot(h, w1s[s], preferred_element_type=jnp.float32).astype(jnp.bfloat16)
            dg_ref[...] = lax.dot_general(e, w2s[s], CONTRACT_LAST, preferred_element_type=jnp.float32).astype(jnp.bfloat16)

        def ew(c, u_ref, dg_ref):
            cols = pl.ds(pl.multiple_of(c * CHUNK, CHUNK), CHUNK)
            u = u_ref[...].astype(jnp.float32)
            sq = u * u
            half = 0.5 + 0.5 * jnp.tanh(u * (GELU_C + (GELU_C * GELU_A) * sq))
            g = (u * half).astype(jnp.bfloat16)
            slope = half + (half - half * half) * (u * (2.0 * GELU_C + (6.0 * GELU_C * GELU_A) * sq))
            du = (dg_ref[...].astype(jnp.float32) * slope).astype(jnp.bfloat16)
            d1 = jnp.dot(hct[...], du, preferred_element_type=jnp.float32)
            d2 = jnp.dot(ect[...], g, preferred_element_type=jnp.float32)
            for k in range(2):
                part[l, 0, k, :, cols] = d1[k * blk:(k + 1) * blk]
                part[l, 1, k, :, cols] = d2[k * blk:(k + 1) * blk]
            if not first:
                finish(l + 1, c)

        def pair(i, c2):
            for n in (1, 2):
                for cp in load_w(li * n_chunks + 2 * i + n):
                    cp.wait()
            for n in (3, 4):
                for cp in load_w(li * n_chunks + 2 * i + n):
                    cp.start()
            mm(2 * i + 1, u_b, dg_b)
            ew(2 * i, u_a, dg_a)
            mm(2 * i + 2, u_a, dg_a)
            ew(2 * i + 1, u_b, dg_b)
            return c2

        if not first:
            swap_wait(l + 1, 0)
        for cp in load_w(li * n_chunks):
            cp.wait()
        for cp in load_w(li * n_chunks + 2):
            cp.start()
        mm(0, u_a, dg_a)
        lax.fori_loop(0, half_chunks // 2, pair, 0)
        swap_start(l, 0)
        if not first:
            swap_wait(l + 1, 1)
        lax.fori_loop(half_chunks // 2, n_chunks // 2, pair, 0)
        ew(n_chunks - 1, u_a, dg_a)
        swap_start(l, 1)
        if not first:
            for cp in put(l + 1):
                cp.start()

    layer_step(0, True)

    def later(li, carry):
        layer_step(li, False)
        return carry

    lax.fori_loop(1, n_layers, later, 0)

    def tail(c, carry):
        finish(0, c)
        return carry

    for cp in put(2):
        cp.wait()
    swap_wait(0, 0)
    lax.fori_loop(0, half_chunks, tail, 0)
    swap_wait(0, 1)
    lax.fori_loop(half_chunks, n_chunks, tail, 0)
    for cp in put(0):
        cp.start()
    for l in (1, 0):
        for cp in put(l):
            cp.wait()
    for q in range(total, total + 2):
        for cp in load_w(q):
            cp.wait()
    for l in range(top):
        for j in range(CHIPS - 1):
            gather(l, j).wait_send()


def run_weights(h_gath, e_own, e_top, w_up, w_down):
    n_layers, _, rows, width = h_gath.shape
    ffn = w_up.shape[2]
    blk = width // (2 * CHIPS)
    bf, f32 = jnp.bfloat16, jnp.float32
    any_spec = pl.BlockSpec(memory_space=pl.ANY)
    dma = pltpu.SemaphoreType.DMA
    return pl.pallas_call(
        weight_kernel,
        out_shape=(
            jax.ShapeDtypeStruct((n_layers, blk, ffn), f32),
            jax.ShapeDtypeStruct((n_layers, ffn, blk), f32),
        ),
        in_specs=[any_spec] * 5,
        out_specs=(any_spec, any_spec),
        scratch_shapes=[
            pltpu.VMEM((n_layers, CHIPS, rows, width), bf),
            pltpu.VMEM((n_layers, CHIPS, rows, width), bf),
            pltpu.VMEM((RING, width, CHUNK), bf),
            pltpu.VMEM((RING, CHUNK, width), bf),
            pltpu.VMEM((2 * blk, CHIPS * rows), bf),
            pltpu.VMEM((2 * blk, CHIPS * rows), bf),
            pltpu.VMEM((CHIPS * rows, CHUNK), bf),
            pltpu.VMEM((CHIPS * rows, CHUNK), bf),
            pltpu.VMEM((CHIPS * rows, CHUNK), bf),
            pltpu.VMEM((CHIPS * rows, CHUNK), bf),
            pltpu.VMEM((n_layers, 2, 2, blk, ffn), f32),
            pltpu.VMEM((n_layers, 2, blk, ffn), f32),
            pltpu.VMEM((2, ffn, blk), f32),
            dma((2, RING)), dma((3,)), dma((3,)), dma((2, 3)),
            dma((2, 3)), dma((2, 3)), dma((3, 2, 2)), dma((3, 2, 2)),
        ],
        compiler_params=pltpu.CompilerParams(collective_id=1, has_side_effects=True, vmem_limit_bytes=67043328),
    )(h_gath, e_own, e_top, w_up, w_down)


def solution(mesh):
    stages = mesh.shape['stage']
    replicas = mesh.shape['data']

    def per_device(x_loc, y_loc, w_up, w_down):
        n_micro, n_tokens, n_width = x_loc.shape
        n_layers = w_up.shape[0]
        rows = n_micro * n_tokens
        total_tokens = replicas * rows
        x_rows = x_loc.reshape(rows, n_width)
        y_rows = y_loc.reshape(rows, n_width)
        h_gath, e_own, e_top, loss = run_chain(x_rows, y_rows, w_up, w_down, stages, total_tokens)
        grad_up, grad_down = run_weights(h_gath, e_own, e_top, w_up, w_down)
        return loss[0, 0], grad_up, grad_down

    return jax.shard_map(
        per_device,
        mesh=mesh,
        in_specs=(P('data', None, None), P('data', None, None), P('stage', None, None), P('stage', None, None)),
        out_specs=(P(), P('stage', 'data', None), P('stage', None, 'data')),
        check_vma=False,
    )
```

```python
import functools

import jax
import jax.numpy as jnp
from jax import lax
from jax.experimental import pallas as pl
from jax.experimental.pallas import tpu as pltpu
from jax.sharding import PartitionSpec as P

CONTRACT_LAST = (((1,), (1,)), ((), ()))
MESH = pl.DeviceIdType.MESH
GELU_C = 0.7978845608028654
GELU_A = 0.044715
CHIPS = 4


def gelu_wide(u):
    th = jnp.tanh(u * (GELU_C + (GELU_C * GELU_A) * (u * u)))
    return u * (0.5 + 0.5 * th)


def gelu_slope(u):
    sq = u * u
    half = 0.5 + 0.5 * jnp.tanh(u * (GELU_C + (GELU_C * GELU_A) * sq))
    return half + (half - half * half) * (u * (2.0 * GELU_C + (6.0 * GELU_C * GELU_A) * sq))


def chain_kernel(stages, total_tokens, x_ref, y_ref, w1_hbm, w2_hbm, h_all, e_out, e_top, loss_ref,
                 w1, w2, ut, g_buf, hs, e_t, e_nat, y_buf, loss_buf, loss_tot,
                 w1_sem, w2_sem, io_sem, hop_send, hop_recv, ag_send, ag_recv, ls_send, ls_recv, turn_sem):
    stage = lax.axis_index('stage')
    data = lax.axis_index('data')
    chip = data // 2
    core = data % 2
    n_layers, width, ffn = w1.shape
    not_first = stage > 0
    not_last = stage < stages - 1
    is_first = jnp.logical_not(not_first)
    is_last = jnp.logical_not(not_last)
    pieces = ((0, 512), (512, width))

    def load_w1(l):
        return pltpu.make_async_copy(w1_hbm.at[l], w1.at[l], w1_sem.at[l])

    def load_w2(l, s):
        return pltpu.make_async_copy(w2_hbm.at[l], w2.at[l % 2], w2_sem.at[s])

    x_copy = pltpu.make_async_copy(x_ref, hs.at[0], io_sem.at[0])
    y_copy = pltpu.make_async_copy(y_ref, y_buf, io_sem.at[1])

    @pl.when(jnp.logical_not(not_first))
    def _():
        x_copy.start()

    load_w1(0).start()

    @pl.when(not_first)
    def _():
        load_w2(0, 0).start()
        load_w1(1).start()
        load_w2(1, 1).start()
        load_w1(2).start()

    @pl.when(jnp.logical_not(not_last))
    def _():
        y_copy.start()

    peers = []
    for j in range(1, CHIPS):
        px = (chip // 2 + j // 2) % 2
        py = (chip % 2 + j % 2) % 2
        peers.append((px * 2 + py) * 2 + core)

    barrier = pltpu.get_barrier_semaphore()
    for k in range(1, 2 * CHIPS):
        pl.semaphore_signal(barrier, inc=1, device_id=(stage, (data + k) % (2 * CHIPS)), device_id_type=MESH)

    @pl.when(not_first)
    def _():
        pl.semaphore_signal(barrier, inc=1, device_id=(stage - 1, data), device_id_type=MESH)

    @pl.when(not_last)
    def _():
        pl.semaphore_signal(barrier, inc=1, device_id=(stage + 1, data), device_id_type=MESH)

    pl.semaphore_wait(barrier, 2 * CHIPS - 1 + jnp.minimum(stage, 1) + jnp.minimum(stages - 1 - stage, 1))

    def hop_up(p):
        lanes = slice(*pieces[p])
        return pltpu.make_async_remote_copy(
            src_ref=hs.at[n_layers, :, lanes], dst_ref=hs.at[0, :, lanes], send_sem=hop_send.at[0, p],
            recv_sem=hop_recv.at[0, p], device_id=(stage + 1, data), device_id_type=MESH)

    def hop_down(p):
        subl = slice(*pieces[p])
        return pltpu.make_async_remote_copy(
            src_ref=e_t.at[0, subl, :], dst_ref=e_t.at[n_layers, subl, :], send_sem=hop_send.at[1, p],
            recv_sem=hop_recv.at[1, p], device_id=(stage - 1, data), device_id_type=MESH)

    def gather(l, j):
        return pltpu.make_async_remote_copy(
            src_ref=hs.at[l], dst_ref=h_all.at[l, chip], send_sem=ag_send.at[l, j], recv_sem=ag_recv.at[l, j],
            device_id=(stage, peers[j]), device_id_type=MESH)

    def keep(l):
        return pltpu.make_async_copy(hs.at[l], h_all.at[l, chip], io_sem.at[2 + l])

    top = n_layers - 1

    def gather_top(j):
        return pltpu.make_async_remote_copy(
            src_ref=e_nat.at[top], dst_ref=e_top.at[chip], send_sem=ag_send.at[n_layers, j],
            recv_sem=ag_recv.at[n_layers, j], device_id=(stage, peers[j]), device_id_type=MESH)

    def keep_e(l):
        dst = e_top.at[chip] if l == top else e_out.at[l]
        return pltpu.make_async_copy(e_nat.at[l], dst, io_sem.at[5 + l])

    def share_loss(k):
        return pltpu.make_async_remote_copy(
            src_ref=loss_buf.at[data], dst_ref=loss_buf.at[data], send_sem=ls_send.at[k - 1], recv_sem=ls_recv.at[k - 1],
            device_id=(stage, (data + k) % (2 * CHIPS)), device_id_type=MESH)

    def loss_down():
        return pltpu.make_async_remote_copy(
            src_ref=loss_tot, dst_ref=loss_tot, send_sem=hop_send.at[2, 0], recv_sem=hop_recv.at[2, 0],
            device_id=(stage - 1, data), device_id_type=MESH)

    @pl.when(not_first)
    def _():
        hop_up(0).wait_recv()
        hop_up(1).wait_recv()

    @pl.when(jnp.logical_and(stage == 1, core == 0))
    def _():
        pl.semaphore_signal(turn_sem, inc=1, device_id=(stage - 1, data), device_id_type=MESH)

    @pl.when(is_first)
    def _():
        x_copy.wait()

    send_now = jnp.logical_and(not_last, jnp.logical_or(not_first, core == 0))

    def fwd_layer(l, carry):
        for j in range(CHIPS - 1):
            gather(l, j).start()
        keep(l).start()
        load_w1(l).wait()

        @pl.when(is_first)
        def _():
            @pl.when(l < top)
            def _():
                load_w2(l, l).start()
        h = hs[l]
        for c in range(ffn // 256):
            cols = slice(c * 256, (c + 1) * 256)
            u = jnp.dot(h, w1[l, :, cols], preferred_element_type=jnp.float32).astype(jnp.bfloat16)
            ut[l, cols, :] = u.T
            g_buf[:, cols] = gelu_wide(u.astype(jnp.float32)).astype(jnp.bfloat16)
        load_w2(l, l).wait()

        @pl.when(is_first)
        def _():
            @pl.when(l < top)
            def _():
                load_w1(l + 1).start()
        for p in range(2):
            lanes = slice(*pieces[p])
            branch = jnp.dot(g_buf[...], w2[l % 2, :, lanes], preferred_element_type=jnp.float32)
            hs[l + 1, :, lanes] = (hs[l, :, lanes].astype(jnp.float32) + branch).astype(jnp.bfloat16)

            @pl.when(jnp.logical_and(l == top, send_now))
            def _():
                hop_up(p).start()

        @pl.when(l == 0)
        def _():
            load_w2(2, 2).start()
        return carry

    lax.fori_loop(0, n_layers, fwd_layer, 0)

    @pl.when(jnp.logical_and(is_first, core == 1))
    def _():
        pl.semaphore_wait(turn_sem, 1)
        hop_up(0).start()
        hop_up(1).start()

    @pl.when(not_last)
    def _():
        hop_up(0).wait_send()
        hop_up(1).wait_send()

    @pl.when(jnp.logical_and(is_first, core == 0))
    def _():
        pl.semaphore_wait(turn_sem, 1)
        pl.semaphore_signal(turn_sem, inc=1, device_id=(stage, data + 1), device_id_type=MESH)

    @pl.when(not_last)
    def _():
        hop_down(0).wait_recv()
        hop_down(1).wait_recv()

    @pl.when(is_last)
    def _():
        y_copy.wait()
        diff = hs[n_layers].astype(jnp.float32) - y_buf[...].astype(jnp.float32)
        e_t[n_layers] = (diff / total_tokens).T.astype(jnp.bfloat16)
        loss_buf[data] = jnp.full((8, 128), jnp.sum(diff * diff), jnp.float32)
        for k in range(1, 2 * CHIPS):
            share_loss(k).start()

    e_nat[top] = e_t[n_layers].T
    for j in range(CHIPS - 1):
        gather_top(j).start()
    keep_e(top).start()
    rows_c = ffn // 19

    def bwd_layer(i, carry):
        l = n_layers - 1 - i

        @pl.when(l == 0)
        def _():
            load_w2(0, 3).wait()
        e_cur = e_t[l + 1]

        @pl.when(l < top)
        def _():
            e_nat[l] = e_t[l + 1].T
        for c in range(19):
            rows = slice(c * rows_c, (c + 1) * rows_c)
            dg = jnp.dot(w2[l % 2, rows, :], e_cur, preferred_element_type=jnp.float32).astype(jnp.bfloat16)
            slope = gelu_slope(ut[l, rows, :].astype(jnp.float32))
            ut[l, rows, :] = (dg.astype(jnp.float32) * slope).astype(jnp.bfloat16)

        @pl.when(l == 2)
        def _():
            load_w2(0, 3).start()

        @pl.when(jnp.logical_or(not_first, l > 0))
        def _():
            for p in range(2):
                subl = slice(*pieces[p])
                back = jnp.dot(w1[l, subl, :], ut[l], preferred_element_type=jnp.float32)
                e_t[l, subl, :] = (e_t[l + 1, subl, :].astype(jnp.float32) + back).astype(jnp.bfloat16)

                @pl.when(l == 0)
                def _():
                    hop_down(p).start()
        return carry

    lax.fori_loop(0, n_layers, bwd_layer, 0)

    for l in range(top):
        keep_e(l).start()

    @pl.when(not_last)
    def _():
        loss_down().wait_recv()

    @pl.when(is_last)
    def _():
        for k in range(1, 2 * CHIPS):
            share_loss(k).wait_send()
            share_loss(k).wait_recv()
        total = loss_buf[0]
        for k in range(1, 2 * CHIPS):
            total = total + loss_buf[k]
        loss_tot[...] = total / (2 * total_tokens)

    loss_ref[...] = loss_tot[...]

    @pl.when(not_first)
    def _():
        loss_down().start()

    for l in range(n_layers):
        keep_e(l).wait()
        keep(l).wait()
        for j in range(CHIPS - 1):
            gather(l, j).wait_send()
            gather(l, j).wait_recv()
    for j in range(CHIPS - 1):
        gather_top(j).wait_send()
        gather_top(j).wait_recv()

    @pl.when(not_first)
    def _():
        hop_down(0).wait_send()
        hop_down(1).wait_send()
        loss_down().wait_send()


def run_chain(x_rows, y_rows, w_up, w_down, stages, total_tokens):
    rows, width = x_rows.shape
    n_layers, _, ffn = w_up.shape
    bf = jnp.bfloat16
    any_spec = pl.BlockSpec(memory_space=pl.ANY)
    return pl.pallas_call(
        functools.partial(chain_kernel, stages, total_tokens),
        out_shape=(
            jax.ShapeDtypeStruct((n_layers, CHIPS, rows, width), bf),
            jax.ShapeDtypeStruct((n_layers - 1, rows, width), bf),
            jax.ShapeDtypeStruct((CHIPS, rows, width), bf),
            jax.ShapeDtypeStruct((8, 128), jnp.float32),
        ),
        in_specs=[any_spec] * 4,
        out_specs=(any_spec, any_spec, any_spec, pl.BlockSpec(memory_space=pltpu.VMEM)),
        scratch_shapes=[
            pltpu.VMEM((n_layers, width, ffn), bf),
            pltpu.VMEM((2, ffn, width), bf),
            pltpu.VMEM((n_layers, ffn, rows), bf),
            pltpu.VMEM((rows, ffn), bf),
            pltpu.VMEM((n_layers + 1, rows, width), bf),
            pltpu.VMEM((n_layers + 1, width, rows), bf),
            pltpu.VMEM((n_layers, rows, width), bf),
            pltpu.VMEM((rows, width), bf),
            pltpu.VMEM((2 * CHIPS, 8, 128), jnp.float32),
            pltpu.VMEM((8, 128), jnp.float32),
            pltpu.SemaphoreType.DMA((3,)),
            pltpu.SemaphoreType.DMA((4,)),
            pltpu.SemaphoreType.DMA((8,)),
            pltpu.SemaphoreType.DMA((3, 2)),
            pltpu.SemaphoreType.DMA((3, 2)),
            pltpu.SemaphoreType.DMA((4, 3)),
            pltpu.SemaphoreType.DMA((4, 3)),
            pltpu.SemaphoreType.DMA((7,)),
            pltpu.SemaphoreType.DMA((7,)),
            pltpu.SemaphoreType.REGULAR,
        ],
        compiler_params=pltpu.CompilerParams(collective_id=0, has_side_effects=True, vmem_limit_bytes=67043328),
    )(x_rows, y_rows, w_up, w_down)


CHUNK = 256
RING = 4


def weight_kernel(h_hbm, e_own, e_top, w1_hbm, w2_hbm, out1, out2,
                  h_buf, e_buf, w1s, w2s, hct, ect, u_a, dg_a, u_b, dg_b, part, recv,
                  w_sem, h_sem, e_sem, o_sem, ag_send, ag_recv, x_send, x_recv):
    stage = lax.axis_index('stage')
    data = lax.axis_index('data')
    chip = data // 2
    core = data % 2
    n_layers, width, ffn = w1_hbm.shape
    n_chunks = ffn // CHUNK
    total = n_layers * n_chunks
    blk = out1.shape[1]
    rows = e_own.shape[1]
    top = n_layers - 1
    partner = data + 1 - 2 * core

    def load_w(q):
        qq = jnp.minimum(q, total - 1)
        l = top - qq // n_chunks
        cols = pl.ds(pl.multiple_of((qq % n_chunks) * CHUNK, CHUNK), CHUNK)
        s = q % RING
        return (pltpu.make_async_copy(w1_hbm.at[l, :, cols], w1s.at[s], w_sem.at[0, s]),
                pltpu.make_async_copy(w2_hbm.at[l, cols, :], w2s.at[s], w_sem.at[1, s]))

    def load_h(l):
        return pltpu.make_async_copy(h_hbm.at[l], h_buf.at[l], h_sem.at[l])

    load_h(top).start()
    top_copy = pltpu.make_async_copy(e_top, e_buf.at[top], e_sem.at[top])
    top_copy.start()
    for q in range(2):
        for cp in load_w(q):
            cp.start()

    peers = []
    for j in range(1, CHIPS):
        px = (chip // 2 + j // 2) % 2
        py = (chip % 2 + j % 2) % 2
        peers.append((px * 2 + py) * 2 + core)
    barrier = pltpu.get_barrier_semaphore()
    for p in peers + [partner]:
        pl.semaphore_signal(barrier, inc=1, device_id=(stage, p), device_id_type=MESH)
    pl.semaphore_wait(barrier, CHIPS)

    def gather(l, j):
        return pltpu.make_async_remote_copy(
            src_ref=e_own.at[l], dst_ref=e_buf.at[l, chip], send_sem=ag_send.at[l, j], recv_sem=ag_recv.at[l, j],
            device_id=(stage, peers[j]), device_id_type=MESH)

    def keep(l):
        return pltpu.make_async_copy(e_own.at[l], e_buf.at[l, chip], e_sem.at[l])

    for l in reversed(range(top)):
        for j in range(CHIPS - 1):
            gather(l, j).start()
        keep(l).start()
        load_h(l).start()

    half_chunks = n_chunks // 2 + 1
    groups = (slice(0, half_chunks * CHUNK), slice(half_chunks * CHUNK, ffn))

    def swap(l, k, p):
        return pltpu.make_async_remote_copy(
            src_ref=part.at[l, k, 1 - core, :, groups[p]], dst_ref=recv.at[l, k, :, groups[p]],
            send_sem=x_send.at[l, k, p], recv_sem=x_recv.at[l, k, p],
            device_id=(stage, partner), device_id_type=MESH)

    def put(l):
        return (pltpu.make_async_copy(part.at[l, 0, core], out1.at[l], o_sem.at[0, l]),
                pltpu.make_async_copy(part.at[l, 1, core], out2.at[l], o_sem.at[1, l]))

    def finish(l, c):
        cols = pl.ds(pl.multiple_of(c * CHUNK, CHUNK), CHUNK)
        for k in range(2):
            part[l, k, core, :, cols] = part[l, k, core, :, cols] + recv[l, k, :, cols]

    def swap_start(l, p):
        for k in range(2):
            swap(l, k, p).start()

    def swap_wait(l, p):
        for k in range(2):
            swap(l, k, p).wait_send()
            swap(l, k, p).wait_recv()

    def layer_step(li, first):
        l = top - li
        load_h(l).wait()
        if first:
            top_copy.wait()
        else:
            keep(l).wait()
            for j in range(CHIPS - 1):
                gather(l, j).wait_recv()

        n_rows = CHIPS * rows
        for k in range(CHIPS):
            @pl.when(chip == k)
            def _():
                lanes = slice(k * 2 * blk, (k + 1) * 2 * blk)
                for r in range(CHIPS):
                    hct[:, r * rows:(r + 1) * rows] = h_buf[l, r, :, lanes].T
                    ect[:, r * rows:(r + 1) * rows] = e_buf[l, r, :, lanes].T

        def mm(c, u_ref, dg_ref):
            q = li * n_chunks + c
            s = q % RING
            h = h_buf[l].reshape(n_rows, width)
            e = e_buf[l].reshape(n_rows, width)
            u_ref[...] = jnp.dot(h, w1s[s], preferred_element_type=jnp.float32).astype(jnp.bfloat16)
            dg_ref[...] = lax.dot_general(e, w2s[s], CONTRACT_LAST, preferred_element_type=jnp.float32).astype(jnp.bfloat16)

        def ew(c, u_ref, dg_ref):
            cols = pl.ds(pl.multiple_of(c * CHUNK, CHUNK), CHUNK)
            u = u_ref[...].astype(jnp.float32)
            sq = u * u
            half = 0.5 + 0.5 * jnp.tanh(u * (GELU_C + (GELU_C * GELU_A) * sq))
            g = (u * half).astype(jnp.bfloat16)
            slope = half + (half - half * half) * (u * (2.0 * GELU_C + (6.0 * GELU_C * GELU_A) * sq))
            du = (dg_ref[...].astype(jnp.float32) * slope).astype(jnp.bfloat16)
            d1 = jnp.dot(hct[...], du, preferred_element_type=jnp.float32)
            d2 = jnp.dot(ect[...], g, preferred_element_type=jnp.float32)
            for k in range(2):
                part[l, 0, k, :, cols] = d1[k * blk:(k + 1) * blk]
                part[l, 1, k, :, cols] = d2[k * blk:(k + 1) * blk]
            if not first:
                finish(l + 1, c)

        def pair(i, c2):
            for n in (1, 2):
                for cp in load_w(li * n_chunks + 2 * i + n):
                    cp.wait()
            for n in (3, 4):
                for cp in load_w(li * n_chunks + 2 * i + n):
                    cp.start()
            mm(2 * i + 1, u_b, dg_b)
            ew(2 * i, u_a, dg_a)
            mm(2 * i + 2, u_a, dg_a)
            ew(2 * i + 1, u_b, dg_b)
            return c2

        if not first:
            swap_wait(l + 1, 0)
        for cp in load_w(li * n_chunks):
            cp.wait()
        for cp in load_w(li * n_chunks + 2):
            cp.start()
        mm(0, u_a, dg_a)
        lax.fori_loop(0, half_chunks // 2, pair, 0)
        swap_start(l, 0)
        if not first:
            swap_wait(l + 1, 1)
        lax.fori_loop(half_chunks // 2, n_chunks // 2, pair, 0)
        ew(n_chunks - 1, u_a, dg_a)
        swap_start(l, 1)
        if not first:
            for cp in put(l + 1):
                cp.start()

    layer_step(0, True)

    def later(li, carry):
        layer_step(li, False)
        return carry

    lax.fori_loop(1, n_layers, later, 0)

    def tail(c, carry):
        finish(0, c)
        return carry

    for cp in put(2):
        cp.wait()
    swap_wait(0, 0)
    lax.fori_loop(0, half_chunks, tail, 0)
    swap_wait(0, 1)
    lax.fori_loop(half_chunks, n_chunks, tail, 0)
    for cp in put(0):
        cp.start()
    for l in (1, 0):
        for cp in put(l):
            cp.wait()
    for q in range(total, total + 2):
        for cp in load_w(q):
            cp.wait()
    for l in range(top):
        for j in range(CHIPS - 1):
            gather(l, j).wait_send()


def run_weights(h_gath, e_own, e_top, w_up, w_down):
    n_layers, _, rows, width = h_gath.shape
    ffn = w_up.shape[2]
    blk = width // (2 * CHIPS)
    bf, f32 = jnp.bfloat16, jnp.float32
    any_spec = pl.BlockSpec(memory_space=pl.ANY)
    dma = pltpu.SemaphoreType.DMA
    return pl.pallas_call(
        weight_kernel,
        out_shape=(
            jax.ShapeDtypeStruct((n_layers, blk, ffn), f32),
            jax.ShapeDtypeStruct((n_layers, blk, ffn), f32),
        ),
        in_specs=[any_spec] * 5,
        out_specs=(any_spec, any_spec),
        scratch_shapes=[
            pltpu.VMEM((n_layers, CHIPS, rows, width), bf),
            pltpu.VMEM((n_layers, CHIPS, rows, width), bf),
            pltpu.VMEM((RING, width, CHUNK), bf),
            pltpu.VMEM((RING, CHUNK, width), bf),
            pltpu.VMEM((2 * blk, CHIPS * rows), bf),
            pltpu.VMEM((2 * blk, CHIPS * rows), bf),
            pltpu.VMEM((CHIPS * rows, CHUNK), bf),
            pltpu.VMEM((CHIPS * rows, CHUNK), bf),
            pltpu.VMEM((CHIPS * rows, CHUNK), bf),
            pltpu.VMEM((CHIPS * rows, CHUNK), bf),
            pltpu.VMEM((n_layers, 2, 2, blk, ffn), f32),
            pltpu.VMEM((n_layers, 2, blk, ffn), f32),
            dma((2, RING)), dma((3,)), dma((3,)), dma((2, 3)),
            dma((2, 3)), dma((2, 3)), dma((3, 2, 2)), dma((3, 2, 2)),
        ],
        compiler_params=pltpu.CompilerParams(collective_id=1, has_side_effects=True, vmem_limit_bytes=67043328),
    )(h_gath, e_own, e_top, w_up, w_down)


def place_kernel(a_hbm, b_hbm, a_out, b_out, a_buf, b_buf, sems):
    n_layers = a_hbm.shape[0]
    ins, outs = [], []
    for l in range(n_layers):
        for k, (src, buf, dst) in enumerate(((a_hbm, a_buf, a_out), (b_hbm, b_buf, b_out))):
            ins.append(pltpu.make_async_copy(src.at[l], buf.at[l], sems.at[0, k, l]))
            outs.append(pltpu.make_async_copy(buf.at[l], dst.at[l], sems.at[1, k, l]))
    for cp in ins:
        cp.start()
    for cp_in, cp_out in zip(ins, outs):
        cp_in.wait()
        cp_out.start()
    for cp in outs:
        cp.wait()


def place(grad_up, grad_down):
    any_spec = pl.BlockSpec(memory_space=pl.ANY)
    return pl.pallas_call(
        place_kernel,
        out_shape=tuple(jax.ShapeDtypeStruct(g.shape, g.dtype) for g in (grad_up, grad_down)),
        in_specs=[any_spec] * 2,
        out_specs=(any_spec, any_spec),
        scratch_shapes=[
            pltpu.VMEM(grad_up.shape, grad_up.dtype),
            pltpu.VMEM(grad_down.shape, grad_down.dtype),
            pltpu.SemaphoreType.DMA((2, 2, grad_up.shape[0])),
        ],
        compiler_params=pltpu.CompilerParams(vmem_limit_bytes=67043328),
    )(grad_up, grad_down)


def solution(mesh):
    stages = mesh.shape['stage']
    replicas = mesh.shape['data']

    def per_device(x_loc, y_loc, w_up, w_down):
        n_micro, n_tokens, n_width = x_loc.shape
        n_layers = w_up.shape[0]
        rows = n_micro * n_tokens
        total_tokens = replicas * rows
        x_rows = x_loc.reshape(rows, n_width)
        y_rows = y_loc.reshape(rows, n_width)
        h_gath, e_own, e_top, loss = run_chain(x_rows, y_rows, w_up, w_down, stages, total_tokens)
        grad_up, grad_down = run_weights(h_gath, e_own, e_top, w_up, w_down)
        grad_up, grad_down = place(grad_up, grad_down)
        return loss[0, 0], grad_up, jnp.swapaxes(grad_down, 1, 2)

    return jax.shard_map(
        per_device,
        mesh=mesh,
        in_specs=(P('data', None, None), P('data', None, None), P('stage', None, None), P('stage', None, None)),
        out_specs=(P(), P('stage', 'data', None), P('stage', None, 'data')),
        check_vma=False,
    )
```
